32 devices in a mesh: bank: 4 (over x, core), zero: 8 (over z, y).
Axes of the slice: x: 2, y: 2, z: 4, core: 2. Of those that a mesh axis runs over, the one named last changes fastest.
Arguments:
- train_gate: float32 [128, 2048, 768], P('bank', 'zero'), may hold values from -0.1875 to 0.1875
- other_gate: bfloat16 [128, 2048, 768], P('bank', 'zero'), may hold values from -0.0625 to 0.0625
- train_up: float32 [128, 2048, 768], P('bank', 'zero'), may hold values from -0.1875 to 0.1875
- other_up: bfloat16 [128, 2048, 768], P('bank', 'zero'), may hold values from -0.0625 to 0.0625
- router_weight: float32 [2048, 128], P('zero', 'bank'), may hold values from -0.125 to 0.125
- router_gain: float32 [2048], P('zero'), may hold values from 0.25 to 1.75
Outputs:
- ready_gate: bfloat16 [128, 2048, 768], P('bank', None, 'zero')
- ready_up: bfloat16 [128, 2048, 768], P('bank', None, 'zero')
- scale_gate: float32 [128, 768], P('bank', 'zero')
- scale_up: float32 [128, 768], P('bank', 'zero')
- serve_router: bfloat16 [2048, 128], replicated
The draws below stay inside these ranges and needn't reach their ends.
All inputs are finite; a program needn't handle non-finite values. Where the reference program divides by a largest or mean magnitude, that divisor is 1e-20 or more.
Results may differ from the reference program's by a relative error of at most 0.001.
Values may be sent and summed in bfloat16 or wider, within the bound.
A program may use at most 256 MiB of HBM per device.

```python
import jax
import jax.numpy as jnp

EXPERTS = 128
D_MODEL = 2048
D_EXPERT = 768


def raised(array, rng, source, target, parts, factor):
    owner, partner = [(jnp.arange(array.shape[axis_at]) // (array.shape[axis_at] // parts)).reshape([-1 if axis == axis_at else 1 for axis in range(array.ndim)]) for axis_at in (source, target)]
    chosen = jax.random.permutation(rng, parts)[partner]
    strong = (owner == chosen) | (owner == (partner + parts // 2) % parts)
    return jnp.where(strong, factor * array, array)


def level_of(rng, extent, pieces, smallest, high):
    factor_of, own = 1.0, jax.random.fold_in(rng, 6)
    for position, blocks in pieces:
        draws = jnp.exp(jax.random.uniform(jax.random.fold_in(own, position), (blocks,), jnp.float32, smallest / len(pieces), high / len(pieces)))
        factor_of = factor_of * jnp.repeat(draws, extent[position] // blocks).reshape([-1 if axis == position else 1 for axis in range(len(extent))])
    return factor_of


def scatter_about(own_key, extent, scale, reach, split=(), dtype=jnp.bfloat16):
    loudness = level_of(own_key, extent, split, -0.22, 0.18) if split else 1.0
    entries = jax.random.normal(own_key, extent, jnp.float32) * scale * loudness
    return jnp.minimum(jnp.maximum(entries, -reach), reach).astype(dtype)


def heavy_noise(rng, dims, width, most, pieces, heavy, held_as=jnp.bfloat16):
    array = width * jax.random.normal(rng, dims, jnp.float32)
    if pieces:
        array = array * level_of(rng, dims, pieces, -0.22, 0.18)
    return jnp.clip(raised(array, jax.random.fold_in(rng, 3), *heavy), -most, most).astype(held_as)


def setup_inputs(seed: int = 0) -> dict:
    arg_keys = jax.random.split(jax.random.key(seed), 7)
    return {
        "train_gate": heavy_noise(arg_keys[0], (EXPERTS, D_MODEL, D_EXPERT), D_MODEL ** -0.5, 0.1875, ((0, 4), (1, 8)), (1, 2, 8, 2.0), jnp.float32),
        "other_gate": scatter_about(arg_keys[1], (EXPERTS, D_MODEL, D_EXPERT), (D_MODEL * 4) ** -0.5, 0.0625, ((0, 4), (1, 8))),
        "train_up": heavy_noise(arg_keys[2], (EXPERTS, D_MODEL, D_EXPERT), D_MODEL ** -0.5, 0.1875, ((0, 4), (1, 8)), (1, 2, 8, 2.0), jnp.float32),
        "other_up": scatter_about(arg_keys[3], (EXPERTS, D_MODEL, D_EXPERT), (D_MODEL * 4) ** -0.5, 0.0625, ((0, 4), (1, 8))),
        "router_weight": scatter_about(arg_keys[4], (D_MODEL, EXPERTS), D_MODEL ** -0.5, 0.125, ((0, 8), (1, 4)), jnp.float32),
        "router_gain": jnp.clip(1.0 + 0.15 * jax.random.normal(arg_keys[5], (D_MODEL,), jnp.float32), 0.25, 1.75),
    }


def reference(train_gate, other_gate, train_up, other_up, router_weight, router_gain):
    latest_gate = train_gate + other_gate.astype(jnp.float32)
    latest_up = train_up + other_up.astype(jnp.float32)
    scale_gate = jnp.max(jnp.abs(latest_gate), axis=1)
    ready_gate = (latest_gate / jnp.expand_dims(scale_gate, 1)).astype(jnp.bfloat16)
    scale_up = jnp.max(jnp.abs(latest_up), axis=1)
    ready_up = (latest_up / jnp.expand_dims(scale_up, 1)).astype(jnp.bfloat16)
    serve_router = (router_weight * router_gain[:, None]).astype(jnp.bfloat16)
    return ready_gate, ready_up, scale_gate, scale_up, serve_router
```

```python
import functools

import jax
import jax.numpy as jnp
from jax import lax
from jax.experimental import pallas as pl
from jax.experimental.pallas import tpu as pltpu
from jax.sharding import PartitionSpec as P

LANES = 128
MAX_SLOTS = 3
SCALE_SLOTS = 3
DIRECT = 3
OUT_PARTS = 8
VMEM_ALL = 63 * 2**20


def exchange(
    n, banks,
    train_gate, other_gate, train_up, other_up, weight, gain,
    ready_gate, ready_up, scale_ref, serve_router,
    max_train, max_other, train_in, other_in, stage, local_max, direct_in, half_in, half_max, cross_in,
    weight_in, gain_in, part_router, router_row,
    max_sem, in_sem, send_sem, recv_sem, direct_send, direct_recv, half_send, half_recv, cross_send, cross_recv,
    gather_send, gather_recv, row_send, row_recv, bank_send, bank_recv, router_sem,
):
    trains, others, readies = (train_gate, train_up), (other_gate, other_up), (ready_gate, ready_up)
    experts, rows, width = train_gate.shape
    piece = width // n
    half = n // 2
    held = half // 2
    batches = experts // held
    me = lax.axis_index("zero")
    place = lax.rem(me, half)
    first = me - place
    offsets = sorted(range(1, n), key=lambda k: abs(2 * k - n))

    def loads(e, train_to, other_to, sem, slots):
        slot = lax.rem(e, slots)
        out = []
        for t in range(2):
            out.append(pltpu.make_async_copy(trains[t].at[e], train_to.at[slot, t], sem.at[slot, t, 0]))
            out.append(pltpu.make_async_copy(others[t].at[e], other_to.at[slot, t], sem.at[slot, t, 1]))
        return out

    def max_loads(e):
        return loads(e, max_train, max_other, max_sem, MAX_SLOTS)

    def scale_loads(e):
        return loads(e, train_in, other_in, in_sem, SCALE_SLOTS)

    def send(src, dst, send_to, recv_to, **device):
        return pltpu.make_async_remote_copy(
            src_ref=src,
            dst_ref=dst,
            send_sem=send_to,
            recv_sem=recv_to,
            device_id=device,
            device_id_type=pl.DeviceIdType.MESH,
        )

    def await_bytes(ref, sem):
        pltpu.make_async_copy(ref, ref, sem).wait()

    def find_max(e):
        slot = lax.rem(e, MAX_SLOTS)
        for copy in max_loads(e):
            copy.wait()
        for t in range(2):
            for at in range(0, width, LANES):
                cols = pl.ds(at, LANES)
                latest = max_train[slot, t, :, cols] + max_other[slot, t, :, cols].astype(jnp.float32)
                local_max[2 * e + t, :, cols] = jnp.max(jnp.abs(latest), axis=0, keepdims=True)

        @pl.when(e + MAX_SLOTS < experts)
        def _():
            for copy in max_loads(e + MAX_SLOTS):
                copy.start()

    def direct_copy(e, k):
        return send(
            local_max.at[pl.ds(2 * e, 2)], direct_in.at[e, k - 1], direct_send.at[k - 1], direct_recv.at[e],
            zero=lax.rem(me + k, n),
        )

    def find_direct(e):
        find_max(e)
        for k in offsets:
            direct_copy(e, k).start()

    def find_batch(b):
        for i in range(held):
            find_max(b * held + i)
        for k in range(1, half):
            at = lax.rem(place + k, half)
            send(
                local_max.at[b * half + at], half_in.at[b, k - 1], half_send.at[k - 1], half_recv.at[b],
                zero=first + at,
            ).start()

    def cross_batch(b):
        await_bytes(half_in.at[b], half_recv.at[b])
        found = local_max[b * half + place]
        for k in range(half - 1):
            found = jnp.maximum(found, half_in[b, k])
        half_max[b] = found
        send(half_max.at[b], cross_in.at[b], cross_send.at[0], cross_recv.at[b], zero=lax.rem(me + half, n)).start()

    def gather_batch(b):
        await_bytes(cross_in.at[b], cross_recv.at[b])
        row = b * half + place
        scale_ref[row] = jnp.maximum(half_max[b], cross_in[b])
        for k in range(1, half):
            at = lax.rem(place + k, half)
            send(
                scale_ref.at[row], scale_ref.at[row], gather_send.at[k - 1], gather_recv.at[b],
                zero=first + at,
            ).start()

    def mine(ref):
        return ref.at[:, :, pl.ds(pl.multiple_of(me * rows, LANES), rows)]

    def data_copy(t, k, e):
        to = lax.rem(me + k, n)
        return send(
            stage.at[t, pl.ds(e, 1), pl.ds(pl.multiple_of(to * piece, 16), piece), :],
            mine(readies[t]).at[pl.ds(e, 1)],
            send_sem.at[t, k - 1],
            recv_sem.at[t, k - 1],
            zero=to,
        )

    def scale_and_send(e):
        slot = lax.rem(e, SCALE_SLOTS)
        for copy in scale_loads(e):
            copy.wait()
        for t in range(2):
            inverse = 1.0 / scale_ref[2 * e + t]
            for at in range(0, width, LANES):
                cols = pl.ds(at, LANES)
                latest = train_in[slot, t, :, cols] + other_in[slot, t, :, cols].astype(jnp.float32)
                narrow = (latest * inverse[:, at:at + LANES]).astype(jnp.bfloat16)
                stage[t, e, cols, :] = narrow.T
            for k in offsets:
                data_copy(t, k, e).start()
        for t in range(2):
            own = stage[t, e, pl.ds(pl.multiple_of(me * piece, 16), piece), :]
            readies[t][e, :, pl.ds(pl.multiple_of(me * rows, LANES), rows)] = own

        @pl.when(e + SCALE_SLOTS < experts)
        def _():
            for copy in scale_loads(e + SCALE_SLOTS):
                copy.start()

    bank = lax.axis_index("bank")
    parts = weight.shape[0]

    def row_copy(k):
        return send(
            part_router,
            router_row.at[:, pl.ds(pl.multiple_of(me * rows, LANES), rows)],
            row_send.at[k - 1],
            row_recv.at[k - 1],
            zero=lax.rem(me + k, n),
        )

    def bank_copy(k):
        return send(
            router_row,
            serve_router.at[pl.ds(pl.multiple_of(bank * parts, 16), parts)],
            bank_send.at[k - 1],
            bank_recv.at[k - 1],
            bank=lax.rem(bank + k, banks),
        )

    for copy in max_loads(0):
        copy.start()
    barrier = pltpu.get_barrier_semaphore()
    for k in offsets:
        pl.semaphore_signal(
            barrier, inc=1, device_id={"zero": lax.rem(me + k, n)}, device_id_type=pl.DeviceIdType.MESH
        )
    for k in range(1, banks):
        pl.semaphore_signal(
            barrier, inc=1, device_id={"bank": lax.rem(bank + k, banks)}, device_id_type=pl.DeviceIdType.MESH
        )
    for e in range(1, MAX_SLOTS):
        for copy in max_loads(e):
            copy.start()
    router_in = (
        pltpu.make_async_copy(weight, weight_in, router_sem.at[0]),
        pltpu.make_async_copy(gain, gain_in, router_sem.at[1]),
    )
    for copy in router_in:
        copy.start()
    pl.semaphore_wait(barrier, n + banks - 2)
    find_direct(0)
    for e in range(SCALE_SLOTS):
        for copy in scale_loads(e):
            copy.start()

    def direct_step(e, carry):
        find_direct(e)
        return carry

    lax.fori_loop(1, DIRECT * held, direct_step, 0)
    for copy in router_in:
        copy.wait()
    part_router[...] = (weight_in[...] * gain_in[...]).astype(jnp.bfloat16)
    router_row[:, pl.ds(pl.multiple_of(me * rows, LANES), rows)] = part_router[...]
    for k in offsets:
        row_copy(k).start()
    find_batch(DIRECT)

    def step(b, carry):
        @pl.when(b >= DIRECT)
        def _():
            await_bytes(scale_ref.at[pl.ds(b * half, half - 1)], gather_recv.at[b])

        def scale_one(i, carry):
            e = b * held + i

            @pl.when(b < DIRECT)
            def _():
                await_bytes(direct_in.at[e], direct_recv.at[e])
                for t in range(2):
                    found = local_max[2 * e + t]
                    for k in range(n - 1):
                        found = jnp.maximum(found, direct_in[e, k, t])
                    scale_ref[2 * e + t] = found

            scale_and_send(e)
            return carry

        lax.fori_loop(0, held, scale_one, 0)

        @pl.when(jnp.logical_and(b + 2 >= DIRECT, b + 2 < batches))
        def _():
            gather_batch(b + 2)

        @pl.when(b + 3 < batches)
        def _():
            cross_batch(b + 3)

        @pl.when(b + 4 < batches)
        def _():
            find_batch(b + 4)

        return carry

    lax.fori_loop(0, batches, step, 0)

    for k in offsets:
        row_copy(k).wait()
    for k in range(1, banks):
        bank_copy(k).start()
    serve_router[pl.ds(pl.multiple_of(bank * parts, 16), parts), :] = router_row[...]
    for k in range(1, banks):
        bank_copy(k).wait()

    rest = batches - DIRECT
    for k in range(1, half):
        await_bytes(local_max.at[pl.ds(0, rest)], half_send.at[k - 1])
        await_bytes(local_max.at[pl.ds(0, rest)], gather_send.at[k - 1])
    await_bytes(local_max.at[pl.ds(0, rest)], cross_send.at[0])
    for k in offsets:
        await_bytes(local_max.at[pl.ds(0, DIRECT * half)], direct_send.at[k - 1])
        to, source = lax.rem(me + k, n), lax.rem(me + n - k, n)
        for t in range(2):
            await_bytes(stage.at[t, :, pl.ds(pl.multiple_of(to * piece, 16), piece), :], send_sem.at[t, k - 1])
            got = readies[t].at[:, :, pl.ds(pl.multiple_of(source * rows, LANES), rows)]
            await_bytes(got, recv_sem.at[t, k - 1])


def finish(
    n, ready_gate, ready_up, scales, router, out_gate, out_up, scale_gate, scale_up, serve_router, turned, sem, small_sem
):
    experts, piece, _ = ready_gate.shape
    me = lax.axis_index("zero")
    count = experts // OUT_PARTS if experts % OUT_PARTS == 0 else experts
    copies = []
    for at in range(0, experts, count):
        for t, (ready, out) in enumerate(((ready_gate, out_gate), (ready_up, out_up))):
            copies.append(pltpu.make_async_copy(ready.at[pl.ds(at, count)], out.at[pl.ds(at, count)], sem.at[t, at // count]))
    for copy in copies:
        copy.start()
    turned[...] = router[...].T
    copies.append(pltpu.make_async_copy(turned, serve_router, small_sem.at[0]))
    copies[-1].start()
    for k in range(n):

        @pl.when(me == k)
        def _():
            scale_gate[...] = scales[:, 0, 0, k * piece:(k + 1) * piece]
            scale_up[...] = scales[:, 1, 0, k * piece:(k + 1) * piece]

    for copy in copies:
        copy.wait()


def by_kernel(n, banks, train_gate, other_gate, train_up, other_up, router_weight, router_gain):
    experts, rows, width = train_gate.shape
    piece = width // n
    parts = router_weight.shape[1]
    anywhere = pl.BlockSpec(memory_space=pltpu.MemorySpace.HBM)
    inside = pl.BlockSpec(memory_space=pltpu.MemorySpace.VMEM)
    ready = pltpu.VMEM((experts, piece, n * rows), jnp.bfloat16)
    half = n // 2
    batches = 2 * experts // half
    outs = (
        ready,
        ready,
        pltpu.VMEM((2 * experts, 1, width), jnp.float32),
        pltpu.VMEM((banks * parts, n * rows), jnp.bfloat16),
    )
    dma = pltpu.SemaphoreType.DMA
    ready_gate, ready_up, scales, router = pl.pallas_call(
        functools.partial(exchange, n, banks),
        out_shape=outs,
        in_specs=[anywhere] * 6,
        out_specs=(inside,) * 4,
        scratch_shapes=[
            pltpu.VMEM((MAX_SLOTS, 2, rows, width), jnp.float32),
            pltpu.VMEM((MAX_SLOTS, 2, rows, width), jnp.bfloat16),
            pltpu.VMEM((SCALE_SLOTS, 2, rows, width), jnp.float32),
            pltpu.VMEM((SCALE_SLOTS, 2, rows, width), jnp.bfloat16),
            pltpu.VMEM((2, experts, width, rows), jnp.bfloat16),
            pltpu.VMEM((2 * experts, 1, width), jnp.float32),
            pltpu.VMEM((DIRECT * half // 2, n - 1, 2, 1, width), jnp.float32),
            pltpu.VMEM((batches, half - 1, 1, width), jnp.float32),
            pltpu.VMEM((batches, 1, width), jnp.float32),
            pltpu.VMEM((batches, 1, width), jnp.float32),
            pltpu.VMEM((parts, rows), jnp.float32),
            pltpu.VMEM((1, rows), jnp.float32),
            pltpu.VMEM((parts, rows), jnp.bfloat16),
            pltpu.VMEM((parts, n * rows), jnp.bfloat16),
            dma((MAX_SLOTS, 2, 2)),
            dma((SCALE_SLOTS, 2, 2)),
            dma((2, n - 1)),
            dma((2, n - 1)),
            dma((n - 1,)),
            dma((DIRECT * half // 2,)),
            dma((half - 1,)),
            dma((batches,)),
            dma((1,)),
            dma((batches,)),
            dma((half - 1,)),
            dma((batches,)),
            dma((n - 1,)),
            dma((n - 1,)),
            dma((banks - 1,)),
            dma((banks - 1,)),
            dma((2,)),
        ],
        compiler_params=pltpu.CompilerParams(
            collective_id=0, has_side_effects=True, vmem_limit_bytes=39 * 2**20
        ),
    )(train_gate, other_gate, train_up, other_up, router_weight.T, router_gain.reshape(1, rows))
    scales = scales.reshape(experts, 2, 1, width)
    out = jax.ShapeDtypeStruct((experts, piece, n * rows), jnp.bfloat16)
    scale = jax.ShapeDtypeStruct((experts, piece), jnp.float32)
    out_gate, out_up, scale_gate, scale_up, serve_router = pl.pallas_call(
        functools.partial(finish, n),
        out_shape=(out, out, scale, scale, jax.ShapeDtypeStruct((n * rows, banks * parts), jnp.bfloat16)),
        in_specs=[inside] * 4,
        out_specs=(anywhere, anywhere, inside, inside, anywhere),
        scratch_shapes=[
            pltpu.VMEM((n * rows, banks * parts), jnp.bfloat16),
            pltpu.SemaphoreType.DMA((2, OUT_PARTS)),
            pltpu.SemaphoreType.DMA((1,)),
        ],
        compiler_params=pltpu.CompilerParams(vmem_limit_bytes=4 * 2**20),
    )(ready_gate, ready_up, scales, router)
    return jnp.swapaxes(out_gate, 1, 2), jnp.swapaxes(out_up, 1, 2), scale_gate, scale_up, serve_router


def by_collectives(train_gate, other_gate, train_up, other_up, part_router):
    latest_gate = train_gate + other_gate.astype(jnp.float32)
    latest_up = train_up + other_up.astype(jnp.float32)
    scale_gate, scale_up = lax.pmax(
        (jnp.max(jnp.abs(latest_gate), axis=1), jnp.max(jnp.abs(latest_up), axis=1)), "zero"
    )
    narrow_gate, narrow_up = (
        (latest_gate / jnp.expand_dims(scale_gate, 1)).astype(jnp.bfloat16),
        (latest_up / jnp.expand_dims(scale_up, 1)).astype(jnp.bfloat16),
    )
    ready_gate, ready_up = (
        lax.all_to_all(narrow_gate, "zero", split_axis=2, concat_axis=1, tiled=True),
        lax.all_to_all(narrow_up, "zero", split_axis=2, concat_axis=1, tiled=True),
    )
    scale_gate = lax.dynamic_slice_in_dim(
        scale_gate, lax.axis_index("zero") * ready_gate.shape[2], ready_gate.shape[2], axis=1
    )
    scale_up = lax.dynamic_slice_in_dim(
        scale_up, lax.axis_index("zero") * ready_up.shape[2], ready_up.shape[2], axis=1
    )
    row_router = lax.all_gather(part_router, "zero", axis=0, tiled=True)
    serve_router = lax.all_gather(row_router, "bank", axis=1, tiled=True)
    return ready_gate, ready_up, scale_gate, scale_up, serve_router


def on_device(n, banks, train_gate, other_gate, train_up, other_up, router_weight, router_gain):
    experts, rows, width = train_gate.shape
    weights = (train_gate, other_gate, train_up, other_up)
    whole_tiles = rows % LANES == 0 and width % LANES == 0 and (width // n) % 16 == 0
    even_parts = n % 4 == 0 and experts % (n // 4) == 0 and router_weight.shape[1] % 16 == 0
    held = 8 * experts * rows * width + (MAX_SLOTS + SCALE_SLOTS) * 12 * rows * width
    held += 4 * width * (8 * experts + DIRECT * n * n)
    if banks > 1 and whole_tiles and even_parts and experts >= 2 * n and held <= VMEM_ALL:
        return by_kernel(n, banks, *weights, router_weight, router_gain)
    return by_collectives(*weights, (router_weight * router_gain[:, None]).astype(jnp.bfloat16))


def solution(mesh):
    return jax.shard_map(
        functools.partial(on_device, mesh.shape["zero"], mesh.shape["bank"]),
        mesh=mesh,
        in_specs=(
            P("bank", "zero", None),
            P("bank", "zero", None),
            P("bank", "zero", None),
            P("bank", "zero", None),
            P("zero", "bank"),
            P("zero"),
        ),
        out_specs=(
            P("bank", None, "zero"),
            P("bank", None, "zero"),
            P("bank", "zero"),
            P("bank", "zero"),
            P(),
        ),
        check_vma=False,
    )
```

```python
import functools

import jax
import jax.numpy as jnp
from jax import lax
from jax.experimental import pallas as pl
from jax.experimental.pallas import tpu as pltpu
from jax.sharding import PartitionSpec as P

LANES = 128
MAX_SLOTS = 3
SCALE_SLOTS = 3
OUT_PARTS = 8
VMEM_ALL = 63 * 2**20


def exchange(
    n, banks,
    train_gate, other_gate, train_up, other_up, weight, gain,
    ready_gate, ready_up, scale_ref, serve_router,
    max_train, max_other, train_in, other_in, stage, local_max, direct_in, half_in, half_max, cross_in,
    weight_in, gain_in, part_router, router_row,
    max_sem, in_sem, send_sem, recv_sem, direct_send, direct_recv, half_send, half_recv, cross_send, cross_recv,
    gather_send, gather_recv, row_send, row_recv, bank_send, bank_recv, router_sem,
):
    trains, others, readies = (train_gate, train_up), (other_gate, other_up), (ready_gate, ready_up)
    experts, rows, width = train_gate.shape
    piece = width // n
    half = n // 2
    held = half // 2
    batches = experts // held
    me = lax.axis_index("zero")
    place = lax.rem(me, half)
    first = me - place
    offsets = sorted(range(1, n), key=lambda k: abs(2 * k - n))

    def loads(e, train_to, other_to, sem, slots):
        slot = lax.rem(e, slots)
        out = []
        for t in range(2):
            out.append(pltpu.make_async_copy(trains[t].at[e], train_to.at[slot, t], sem.at[slot, t, 0]))
            out.append(pltpu.make_async_copy(others[t].at[e], other_to.at[slot, t], sem.at[slot, t, 1]))
        return out

    def max_loads(e):
        return loads(e, max_train, max_other, max_sem, MAX_SLOTS)

    def scale_loads(e):
        return loads(e, train_in, other_in, in_sem, SCALE_SLOTS)

    def send(src, dst, send_to, recv_to, **device):
        return pltpu.make_async_remote_copy(
            src_ref=src,
            dst_ref=dst,
            send_sem=send_to,
            recv_sem=recv_to,
            device_id=device,
            device_id_type=pl.DeviceIdType.MESH,
        )

    def await_bytes(ref, sem):
        pltpu.make_async_copy(ref, ref, sem).wait()

    def find_max(e):
        slot = lax.rem(e, MAX_SLOTS)
        copies = max_loads(e)
        for t in range(2):
            for copy in copies[2 * t:2 * t + 2]:
                copy.wait()
            for at in range(0, width, LANES):
                cols = pl.ds(at, LANES)
                latest = max_train[slot, t, :, cols] + max_other[slot, t, :, cols].astype(jnp.float32)
                local_max[2 * e + t, :, cols] = jnp.max(jnp.abs(latest), axis=0, keepdims=True)

        @pl.when(e + MAX_SLOTS < experts)
        def _():
            for copy in max_loads(e + MAX_SLOTS):
                copy.start()

    def direct_copy(e, k):
        return send(
            local_max.at[pl.ds(2 * e, 2)], direct_in.at[e, k - 1], direct_send.at[k - 1], direct_recv.at[e],
            zero=lax.rem(me + k, n),
        )

    def send_direct(e):
        for k in offsets:
            direct_copy(e, k).start()

    def find_batch(b):
        for i in range(held):
            find_max(b * held + i)
        for k in range(1, half):
            at = lax.rem(place + k, half)
            send(
                local_max.at[b * half + at], half_in.at[b, k - 1], half_send.at[k - 1], half_recv.at[b],
                zero=first + at,
            ).start()

    def cross_batch(b):
        await_bytes(half_in.at[b], half_recv.at[b])
        found = local_max[b * half + place]
        for k in range(half - 1):
            found = jnp.maximum(found, half_in[b, k])
        half_max[b] = found
        send(half_max.at[b], cross_in.at[b], cross_send.at[0], cross_recv.at[b], zero=lax.rem(me + half, n)).start()

    def gather_batch(b):
        await_bytes(cross_in.at[b], cross_recv.at[b])
        row = b * half + place
        scale_ref[row] = jnp.maximum(half_max[b], cross_in[b])
        for k in range(1, half):
            at = lax.rem(place + k, half)
            send(
                scale_ref.at[row], scale_ref.at[row], gather_send.at[k - 1], gather_recv.at[b],
                zero=first + at,
            ).start()

    def mine(ref):
        return ref.at[:, :, pl.ds(pl.multiple_of(me * rows, LANES), rows)]

    def data_copy(t, k, some):
        to = lax.rem(me + k, n)
        return send(
            stage.at[t, some, pl.ds(pl.multiple_of(to * piece, 16), piece), :],
            mine(readies[t]).at[some],
            send_sem.at[t, k - 1],
            recv_sem.at[t, k - 1],
            zero=to,
        )

    def scale_and_send(e):
        slot = lax.rem(e, SCALE_SLOTS)
        copies = scale_loads(e)
        for t in range(2):
            for copy in copies[2 * t:2 * t + 2]:
                copy.wait()
            inverse = 1.0 / scale_ref[2 * e + t]
            for at in range(0, width, LANES):
                cols = pl.ds(at, LANES)
                latest = train_in[slot, t, :, cols] + other_in[slot, t, :, cols].astype(jnp.float32)
                narrow = (latest * inverse[:, at:at + LANES]).astype(jnp.bfloat16)
                stage[t, e, cols, :] = narrow.T

            @pl.when(e < held)
            def _():
                for k in offsets:
                    data_copy(t, k, pl.ds(e, 1)).start()

            @pl.when(jnp.logical_and(e >= held, lax.rem(e, held) == held - 1))
            def _():
                for k in offsets:
                    data_copy(t, k, pl.ds(e - held + 1, held)).start()

        for t in range(2):
            own = stage[t, e, pl.ds(pl.multiple_of(me * piece, 16), piece), :]
            readies[t][e, :, pl.ds(pl.multiple_of(me * rows, LANES), rows)] = own

        @pl.when(e + SCALE_SLOTS < experts)
        def _():
            for copy in scale_loads(e + SCALE_SLOTS):
                copy.start()

    bank = lax.axis_index("bank")
    parts = weight.shape[0]

    partner = lax.rem(me + half, n)

    def row_block(ref, owner):
        return ref.at[:, pl.ds(pl.multiple_of(owner * rows, LANES), rows)]

    def row_copies():
        out = []
        for k in range(1, half + 1):
            to = partner if k == half else first + lax.rem(place + k, half)
            out.append(send(part_router, row_block(router_row, me), row_send.at[k - 1], row_recv.at[k - 1], zero=to))
        return out

    def pass_on_copies():
        block = row_block(router_row, partner)
        out = []
        for k in range(1, half):
            to = first + lax.rem(place + k, half)
            out.append(send(block, block, row_send.at[half + k - 1], row_recv.at[half + k - 1], zero=to))
        return out

    def bank_copy(k):
        return send(
            router_row,
            serve_router.at[pl.ds(pl.multiple_of(bank * parts, 16), parts)],
            bank_send.at[k - 1],
            bank_recv.at[k - 1],
            bank=lax.rem(bank + k, banks),
        )

    for copy in max_loads(0):
        copy.start()
    barrier = pltpu.get_barrier_semaphore()
    for k in offsets:
        pl.semaphore_signal(
            barrier, inc=1, device_id={"zero": lax.rem(me + k, n)}, device_id_type=pl.DeviceIdType.MESH
        )
    for k in range(1, banks):
        pl.semaphore_signal(
            barrier, inc=1, device_id={"bank": lax.rem(bank + k, banks)}, device_id_type=pl.DeviceIdType.MESH
        )
    router_in = (
        pltpu.make_async_copy(weight, weight_in, router_sem.at[0]),
        pltpu.make_async_copy(gain, gain_in, router_sem.at[1]),
    )
    for copy in router_in:
        copy.start()
    find_max(0)
    pl.semaphore_wait(barrier, n + banks - 2)
    send_direct(0)
    for e in range(1, MAX_SLOTS):
        for copy in max_loads(e):
            copy.start()
    for copy in scale_loads(0):
        copy.start()
    for copy in router_in:
        copy.wait()
    part_router[...] = (weight_in[...] * gain_in[...]).astype(jnp.bfloat16)
    row_block(router_row, me)[...] = part_router[...]
    for e in range(1, held):
        find_max(e)
        send_direct(e)
    for copy in row_copies():
        copy.start()
    for e in range(1, SCALE_SLOTS):
        for copy in scale_loads(e):
            copy.start()

    def scale_one(e, carry):
        @pl.when(e < held)
        def _():
            await_bytes(direct_in.at[e], direct_recv.at[e])
            for t in range(2):
                found = local_max[2 * e + t]
                for k in range(n - 1):
                    found = jnp.maximum(found, direct_in[e, k, t])
                scale_ref[2 * e + t] = found

        scale_and_send(e)
        return carry

    find_batch(1)
    find_batch(2)
    cross_batch(1)
    scale_one(0, 0)
    find_batch(3)
    gather_batch(1)
    cross_batch(2)

    def step(b, carry):
        @pl.when(b >= 1)
        def _():
            await_bytes(scale_ref.at[pl.ds(b * half, half - 1)], gather_recv.at[b])

        lax.fori_loop(jnp.maximum(b * held, 1), (b + 1) * held, scale_one, 0)

        @pl.when(b == 2)
        def _():
            row_copies()[half - 1].wait_recv()
            for copy in pass_on_copies():
                copy.start()

        @pl.when(b + 2 < batches)
        def _():
            gather_batch(b + 2)

        @pl.when(b + 3 < batches)
        def _():
            cross_batch(b + 3)

        @pl.when(b + 4 < batches)
        def _():
            find_batch(b + 4)

        return carry

    lax.fori_loop(0, batches, step, 0)

    rows_in = row_copies()
    for copy in rows_in[:half - 1] + pass_on_copies():
        copy.wait()
    rows_in[half - 1].wait_send()
    for k in range(1, banks):
        bank_copy(k).start()
    serve_router[pl.ds(pl.multiple_of(bank * parts, 16), parts), :] = router_row[...]
    for k in range(1, banks):
        bank_copy(k).wait()

    rest = batches - 1
    for k in range(1, half):
        await_bytes(local_max.at[pl.ds(0, rest)], half_send.at[k - 1])
        await_bytes(local_max.at[pl.ds(0, rest)], gather_send.at[k - 1])
    await_bytes(local_max.at[pl.ds(0, rest)], cross_send.at[0])
    for k in offsets:
        await_bytes(local_max.at[pl.ds(0, half)], direct_send.at[k - 1])
        to, source = lax.rem(me + k, n), lax.rem(me + n - k, n)
        for t in range(2):
            await_bytes(stage.at[t, :, pl.ds(pl.multiple_of(to * piece, 16), piece), :], send_sem.at[t, k - 1])
            got = readies[t].at[:, :, pl.ds(pl.multiple_of(source * rows, LANES), rows)]
            await_bytes(got, recv_sem.at[t, k - 1])


def finish(
    n, ready_gate, ready_up, scales, router, out_gate, out_up, out_scale_gate, out_scale_up, serve_router,
    scale_gate, scale_up, turned, sem, small_sem,
):
    experts, piece, _ = ready_gate.shape
    me = lax.axis_index("zero")
    count = experts // OUT_PARTS
    copies = []
    for i in range(OUT_PARTS):
        some = pl.ds(i * count, count)
        for t, (ready, out) in enumerate(((ready_gate, out_gate), (ready_up, out_up))):
            copies.append(pltpu.make_async_copy(ready.at[some], out.at[some], sem.at[t, i]))
    for copy in copies:
        copy.start()
    turned[...] = router[...].T
    for k in range(n):

        @pl.when(me == k)
        def _():
            scale_gate[...] = scales[:, 0, 0, k * piece:(k + 1) * piece]
            scale_up[...] = scales[:, 1, 0, k * piece:(k + 1) * piece]

    small = ((turned, serve_router), (scale_gate, out_scale_gate), (scale_up, out_scale_up))
    for i, (source, target) in enumerate(small):
        copies.append(pltpu.make_async_copy(source, target, small_sem.at[i]))
        copies[-1].start()
    for copy in copies:
        copy.wait()


def by_kernel(n, banks, train_gate, other_gate, train_up, other_up, router_weight, router_gain):
    experts, rows, width = train_gate.shape
    piece = width // n
    parts = router_weight.shape[1]
    anywhere = pl.BlockSpec(memory_space=pltpu.MemorySpace.HBM)
    inside = pl.BlockSpec(memory_space=pltpu.MemorySpace.VMEM)
    ready = pltpu.VMEM((experts, piece, n * rows), jnp.bfloat16)
    half = n // 2
    batches = 2 * experts // half
    outs = (
        ready,
        ready,
        pltpu.VMEM((2 * experts, 1, width), jnp.float32),
        pltpu.VMEM((banks * parts, n * rows), jnp.bfloat16),
    )
    dma = pltpu.SemaphoreType.DMA
    ready_gate, ready_up, scales, router = pl.pallas_call(
        functools.partial(exchange, n, banks),
        out_shape=outs,
        in_specs=[anywhere] * 6,
        out_specs=(inside,) * 4,
        scratch_shapes=[
            pltpu.VMEM((MAX_SLOTS, 2, rows, width), jnp.float32),
            pltpu.VMEM((MAX_SLOTS, 2, rows, width), jnp.bfloat16),
            pltpu.VMEM((SCALE_SLOTS, 2, rows, width), jnp.float32),
            pltpu.VMEM((SCALE_SLOTS, 2, rows, width), jnp.bfloat16),
            pltpu.VMEM((2, experts, width, rows), jnp.bfloat16),
            pltpu.VMEM((2 * experts, 1, width), jnp.float32),
            pltpu.VMEM((half // 2, n - 1, 2, 1, width), jnp.float32),
            pltpu.VMEM((batches, half - 1, 1, width), jnp.float32),
            pltpu.VMEM((batches, 1, width), jnp.float32),
            pltpu.VMEM((batches, 1, width), jnp.float32),
            pltpu.VMEM((parts, rows), jnp.float32),
            pltpu.VMEM((1, rows), jnp.float32),
            pltpu.VMEM((parts, rows), jnp.bfloat16),
            pltpu.VMEM((parts, n * rows), jnp.bfloat16),
            dma((MAX_SLOTS, 2, 2)),
            dma((SCALE_SLOTS, 2, 2)),
            dma((2, n - 1)),
            dma((2, n - 1)),
            dma((n - 1,)),
            dma((half // 2,)),
            dma((half - 1,)),
            dma((batches,)),
            dma((1,)),
            dma((batches,)),
            dma((half - 1,)),
            dma((batches,)),
            dma((n - 1,)),
            dma((n - 1,)),
            dma((banks - 1,)),
            dma((banks - 1,)),
            dma((2,)),
        ],
        compiler_params=pltpu.CompilerParams(
            collective_id=0, has_side_effects=True, vmem_limit_bytes=39 * 2**20
        ),
    )(train_gate, other_gate, train_up, other_up, router_weight.T, router_gain.reshape(1, rows))
    scales = scales.reshape(experts, 2, 1, width)
    out = jax.ShapeDtypeStruct((experts, piece, n * rows), jnp.bfloat16)
    scale = jax.ShapeDtypeStruct((experts, piece), jnp.float32)
    out_gate, out_up, scale_gate, scale_up, serve_router = pl.pallas_call(
        functools.partial(finish, n),
        out_shape=(out, out, scale, scale, jax.ShapeDtypeStruct((n * rows, banks * parts), jnp.bfloat16)),
        in_specs=[inside] * 4,
        out_specs=(anywhere,) * 5,
        scratch_shapes=[
            pltpu.VMEM((experts, piece), jnp.float32),
            pltpu.VMEM((experts, piece), jnp.float32),
            pltpu.VMEM((n * rows, banks * parts), jnp.bfloat16),
            pltpu.SemaphoreType.DMA((2, OUT_PARTS)),
            pltpu.SemaphoreType.DMA((3,)),
        ],
        compiler_params=pltpu.CompilerParams(vmem_limit_bytes=4 * 2**20),
    )(ready_gate, ready_up, scales, router)
    return jnp.swapaxes(out_gate, 1, 2), jnp.swapaxes(out_up, 1, 2), scale_gate, scale_up, serve_router


def by_collectives(train_gate, other_gate, train_up, other_up, part_router):
    latest_gate = train_gate + other_gate.astype(jnp.float32)
    latest_up = train_up + other_up.astype(jnp.float32)
    scale_gate, scale_up = lax.pmax(
        (jnp.max(jnp.abs(latest_gate), axis=1), jnp.max(jnp.abs(latest_up), axis=1)), "zero"
    )
    narrow_gate, narrow_up = (
        (latest_gate / jnp.expand_dims(scale_gate, 1)).astype(jnp.bfloat16),
        (latest_up / jnp.expand_dims(scale_up, 1)).astype(jnp.bfloat16),
    )
    ready_gate, ready_up = (
        lax.all_to_all(narrow_gate, "zero", split_axis=2, concat_axis=1, tiled=True),
        lax.all_to_all(narrow_up, "zero", split_axis=2, concat_axis=1, tiled=True),
    )
    scale_gate = lax.dynamic_slice_in_dim(
        scale_gate, lax.axis_index("zero") * ready_gate.shape[2], ready_gate.shape[2], axis=1
    )
    scale_up = lax.dynamic_slice_in_dim(
        scale_up, lax.axis_index("zero") * ready_up.shape[2], ready_up.shape[2], axis=1
    )
    row_router = lax.all_gather(part_router, "zero", axis=0, tiled=True)
    serve_router = lax.all_gather(row_router, "bank", axis=1, tiled=True)
    return ready_gate, ready_up, scale_gate, scale_up, serve_router


def on_device(n, banks, train_gate, other_gate, train_up, other_up, router_weight, router_gain):
    experts, rows, width = train_gate.shape
    weights = (train_gate, other_gate, train_up, other_up)
    whole_tiles = rows % LANES == 0 and width % LANES == 0 and (width // n) % 16 == 0
    even_parts = n % 4 == 0 and experts % (n // 4) == 0 and router_weight.shape[1] % 16 == 0
    held = 8 * experts * rows * width + (MAX_SLOTS + SCALE_SLOTS) * 12 * rows * width
    held += 4 * width * (8 * experts + n * n)
    if banks > 1 and whole_tiles and even_parts and experts >= 2 * n and experts % OUT_PARTS == 0 and held <= VMEM_ALL:
        return by_kernel(n, banks, *weights, router_weight, router_gain)
    return by_collectives(*weights, (router_weight * router_gain[:, None]).astype(jnp.bfloat16))


def solution(mesh):
    return jax.shard_map(
        functools.partial(on_device, mesh.shape["zero"], mesh.shape["bank"]),
        mesh=mesh,
        in_specs=(
            P("bank", "zero", None),
            P("bank", "zero", None),
            P("bank", "zero", None),
            P("bank", "zero", None),
            P("zero", "bank"),
            P("zero"),
        ),
        out_specs=(
            P("bank", None, "zero"),
            P("bank", None, "zero"),
            P("bank", "zero"),
            P("bank", "zero"),
            P(),
        ),
        check_vma=False,
    )
```
